32 devices in a mesh: dof: 16 (over z, x, core), mode: 2 (over y).
Axes of the slice: x: 2, y: 2, z: 4, core: 2. Of those that a mesh axis runs over, the one named last changes fastest.
Arguments:
- stiffness_tiles: bfloat16 [512, 10, 128, 128], P('dof'), may hold values from -0.15625 to 0.15625
- tile_cols: int32 [512, 10], P('dof'), may hold values from 0 to 47, as said below
- send_rows: int32 [32, 8], P('dof'), may hold values from 0 to 31, as said below
- block: bfloat16 [65536, 128], P('dof', 'mode'), may hold values from -51 to 51
- lower_bound: float32 [1], replicated, may hold values from -1.2 to -0.6
- upper_bound: float32 [1], replicated, may hold values from 0.4 to 0.9
Outputs:
- basis: bfloat16 [65536, 128], P('dof', 'mode')
- ritz: float32 [128, 128], replicated
The draws below stay inside these ranges and needn't reach their ends.
Inputs may be any that keep to these rules, and one draw needn't show every extreme that they name: `tile_cols`: entry 0 of every tile row is that row's own local index; entry 1 is a code of the lower neighbour's upward list and entry 2 a code of the upper neighbour's downward list. A code below 32 is a tile row of the same partition; 32 + s is slot s of the lower neighbour's upward list; 40 + s is slot s of the upper neighbour's downward list. `send_rows`: rows 2 p and 2 p + 1 hold distinct local tile rows of partition p: its downward and upward send lists.
All inputs are finite; a program needn't handle non-finite values.
Results may differ from the reference program's by a relative error of at most 0.0086.
Values may be sent and summed in bfloat16 or wider, within the bound.
A program may use at most 64 MiB of HBM per device.

```python
import jax
import jax.numpy as jnp
from jax import lax

TILE = 128
MODES = 128
NNZ = 10
DEGREE = 2
ROWT = 32
NSEND = 8
TROWS = 512
NDOF = 65536


def draw_block(key, part):
    key_base = jax.random.fold_in(key, 0)
    key_common = jax.random.fold_in(key, 2)
    key_weights = jax.random.fold_in(key, 3)
    shared_count = 8
    row_index = jnp.arange(NDOF, dtype=jnp.float32)[:, None]
    row_rise = 1.0 + 2.0 * row_index / NDOF
    mixing = jnp.clip(jax.random.normal(key_weights, (shared_count, MODES), jnp.float32), -4.0, 4.0)
    base_draw = jnp.clip(jax.random.normal(key_base, (NDOF, MODES), jnp.float32), -6.0, 6.0)
    common = jnp.clip(jax.random.normal(key_common, (NDOF, shared_count), jnp.float32), -4.0, 4.0)
    shared = 0.45 * jnp.dot(common, mixing, precision=lax.Precision.HIGHEST)
    values = (base_draw + shared) * row_rise
    return jnp.clip(values, -51.0, 51.0).astype(jnp.bfloat16)


def draw_tile_cols(key, part):
    key_pick, key_local, key_ghost, key_low, key_up = jax.random.split(key, 5)
    local_col = jax.random.randint(key_local, (TROWS, NNZ), 0, ROWT)
    ghost_col = jax.random.randint(key_ghost, (TROWS, NNZ), ROWT, ROWT + 2 * NSEND)
    chooser = jax.random.randint(key_pick, (TROWS, NNZ), 0, 10)
    picked = jnp.where(chooser < 3, ghost_col, local_col)
    low_col = jax.random.randint(key_low, (TROWS, NNZ), ROWT, ROWT + NSEND)
    up_col = jax.random.randint(key_up, (TROWS, NNZ), ROWT + NSEND, ROWT + 2 * NSEND)
    own_row = (jnp.arange(TROWS, dtype=jnp.int32) % ROWT)[:, None]
    column = jnp.arange(NNZ, dtype=jnp.int32)[None, :]
    picked = jnp.where(column == 1, low_col, jnp.where(column == 2, up_col, picked))
    return jnp.where(column == 0, own_row, picked).astype(jnp.int32)


def draw_send_rows(key, part):
    list_count = 2 * (TROWS // ROWT)
    scores = jax.random.randint(key, (list_count, ROWT), 0, 1 << 20) * ROWT + jnp.arange(ROWT, dtype=jnp.int32)[None, :]
    ordering = jnp.argsort(scores, axis=-1, stable=True)
    return ordering[:, :NSEND].astype(jnp.int32)


def shard_levels(key, shape, cuts, least, high):
    level, own = 1.0, jax.random.fold_in(key, 6)
    for dim, shards_of in cuts:
        heights = jnp.exp(jax.random.uniform(jax.random.fold_in(own, dim), (shards_of,), jnp.float32, least / len(cuts), high / len(cuts)))
        level = level * jnp.repeat(heights, shape[dim] // shards_of).reshape([-1 if axis == dim else 1 for axis in range(len(shape))])
    return level


def noise(rng, dims, width, reach, cuts=(), held_as=jnp.bfloat16):
    loudness = shard_levels(rng, dims, cuts, -0.22, 0.18) if cuts else 1.0
    values = jax.random.normal(rng, dims, jnp.float32) * width * loudness
    return jnp.minimum(jnp.maximum(values, -reach), reach).astype(held_as)


def setup_inputs(seed: int = 0) -> dict:
    splits = jax.random.split(jax.random.key(seed), 7)
    return {
        "stiffness_tiles": noise(splits[0], (TROWS, NNZ, TILE, TILE), (NNZ * TILE) ** -0.5, 0.15625, ((0, 16),)),
        "tile_cols": draw_tile_cols(jax.random.fold_in(splits[6], 71), 0),
        "send_rows": draw_send_rows(jax.random.fold_in(splits[6], 71), 0),
        "block": draw_block(jax.random.fold_in(splits[6], 71), 0),
        "lower_bound": jnp.clip(jax.random.uniform(splits[4], (1,), jnp.float32, -1.2, -0.6), -1.2, -0.6),
        "upper_bound": jnp.clip(jax.random.uniform(splits[5], (1,), jnp.float32, 0.4, 0.9), 0.4, 0.9),
    }


def apply_stiffness(stiffness_tiles, tile_cols, send_rows, field):
    part_count = TROWS // ROWT
    tile_view = field.reshape(TROWS, TILE, MODES)

    def partition_product(part_index):
        col_code = lax.dynamic_slice_in_dim(tile_cols, part_index * ROWT, ROWT, 0)
        lower_part = jnp.maximum(part_index - 1, 0).astype(jnp.int32)
        upper_part = jnp.minimum(part_index + 1, part_count - 1).astype(jnp.int32)
        low_rows = lax.dynamic_index_in_dim(send_rows, 2 * lower_part + 1, 0, keepdims=False)
        up_rows = lax.dynamic_index_in_dim(send_rows, 2 * upper_part, 0, keepdims=False)
        low_slot = jnp.clip(col_code - ROWT, 0, NSEND - 1)
        up_slot = jnp.clip(col_code - ROWT - NSEND, 0, NSEND - 1)
        source_row = jnp.where(col_code < ROWT, part_index * ROWT + col_code, jnp.where(col_code < ROWT + NSEND, lower_part * ROWT + low_rows[low_slot], upper_part * ROWT + up_rows[up_slot])).astype(jnp.int32)
        present = jnp.where(col_code < ROWT, True, jnp.where(col_code < ROWT + NSEND, part_index > 0, part_index < part_count - 1))
        blocks = tile_view[source_row].astype(jnp.float32) * present[:, :, None, None].astype(jnp.float32)
        row_tiles = lax.dynamic_slice_in_dim(stiffness_tiles, part_index * ROWT, ROWT, 0).astype(jnp.float32)
        return jnp.einsum('rkij,rkjm->rim', row_tiles, blocks)
    result = lax.map(partition_product, jnp.arange(part_count, dtype=jnp.int32))
    return result.reshape(NDOF, MODES)

def reference(stiffness_tiles, tile_cols, send_rows, block, lower_bound, upper_bound):
    center = (upper_bound[0] + lower_bound[0]) * 0.5
    half_width = (upper_bound[0] - lower_bound[0]) * 0.5
    previous = block
    current = ((apply_stiffness(stiffness_tiles, tile_cols, send_rows, block) - center * block.astype(jnp.float32)) / half_width).astype(jnp.bfloat16)
    for step in range(DEGREE - 1):
        following = (2.0 * (apply_stiffness(stiffness_tiles, tile_cols, send_rows, current) - center * current.astype(jnp.float32)) / half_width - previous.astype(jnp.float32)).astype(jnp.bfloat16)
        previous, current = (current, following)
    filtered = current
    image_block = apply_stiffness(stiffness_tiles, tile_cols, send_rows, filtered).astype(jnp.bfloat16)
    gram_matrix = jnp.dot(filtered.T.astype(jnp.float32), filtered.astype(jnp.float32), preferred_element_type=jnp.float32) / NDOF
    projected = jnp.dot(filtered.T.astype(jnp.float32), image_block.astype(jnp.float32), preferred_element_type=jnp.float32) / NDOF
    factor = jnp.linalg.cholesky(gram_matrix)
    identity = jnp.eye(MODES, dtype=jnp.float32)
    inverse = jax.scipy.linalg.solve_triangular(factor, identity, lower=True)
    ritz_matrix = jnp.dot(jnp.dot(inverse, projected, precision=lax.Precision.HIGHEST), inverse.T, precision=lax.Precision.HIGHEST)
    right_factor = inverse.T.astype(jnp.bfloat16)
    basis_out = jnp.dot(filtered.astype(jnp.float32), right_factor.astype(jnp.float32), preferred_element_type=jnp.float32).astype(jnp.bfloat16)
    return (basis_out, ritz_matrix)
```

```python
import functools

import jax
import jax.numpy as jnp
from jax import lax
from jax.experimental import pallas as pl
from jax.experimental.pallas import tpu as pltpu
from jax.sharding import PartitionSpec as P

MESH = pl.DeviceIdType.MESH
NT = (((1,), (1,)), ((), ()))
NN = (((1,), (0,)), ((), ()))
TN = (((0,), (0,)), ((), ()))
EXACT = lax.Precision.HIGHEST


def kernel(
    parts, cols, rows, low_ref, high_ref, x_ref, a_hbm, basis_ref, ritz_ref,
    a_ref, level0, level1, level2, plain, image, other, sends, ar_send, ar_recv,
    work, inv_ref, inv_t,
    a_sem, halo_send, halo_recv, mode_send, mode_recv, ar_ssem, ar_rsem,
):
    tiles, nnz, size = a_ref.shape[0], a_ref.shape[1], a_ref.shape[2]
    modes = x_ref.shape[0]
    width = 2 * modes
    slots = rows.shape[1]
    stages = ar_send.shape[0] - 1
    chunks = mode_send.shape[0]
    part_rows = tiles // chunks
    p = lax.axis_index("dof")
    my = lax.axis_index("mode")
    has_low = p > 0
    has_up = p < parts - 1

    loads = []
    a_parts = a_sem.shape[0]
    for i in range(a_parts):
        span = pl.ds(i * (tiles // a_parts), tiles // a_parts)
        loads.append(pltpu.make_async_copy(a_hbm.at[span], a_ref.at[span], a_sem.at[i]))
        loads[-1].start()

    def flipped(bit):
        return p + bit * (1 - 2 * ((p // bit) % 2))

    barrier = pltpu.get_barrier_semaphore()
    for s in range(stages):
        pl.semaphore_signal(barrier, inc=1, device_id=(flipped(1 << s), my), device_id_type=MESH)
    pl.semaphore_signal(barrier, inc=1, device_id=(p, 1 - my), device_id_type=MESH)

    @pl.when(has_low)
    def _():
        pl.semaphore_signal(barrier, inc=1, device_id=(p - 1, my), device_id_type=MESH)

    @pl.when(has_up)
    def _():
        pl.semaphore_signal(barrier, inc=1, device_id=(p + 1, my), device_id_type=MESH)

    for t in range(tiles):
        tile = x_ref[:, t * size : (t + 1) * size]
        level0[t] = tile
        plain[t] = tile

    @pl.when(p == 0)
    def _():
        for level in (level0, level1, level2):
            level[tiles : tiles + slots] = jnp.zeros((slots, modes, size), jnp.bfloat16)

    @pl.when(p == parts - 1)
    def _():
        for level in (level0, level1, level2):
            level[tiles + slots :] = jnp.zeros((slots, modes, size), jnp.bfloat16)

    for s in range(slots):
        sends[0, s] = plain[rows[1, s]]
        sends[0, slots + s] = plain[rows[0, s]]

    pl.semaphore_wait(
        barrier, stages + 1 + has_low.astype(jnp.int32) + has_up.astype(jnp.int32)
    )

    def halo(index, level):
        up = pltpu.make_async_remote_copy(
            src_ref=sends.at[index, pl.ds(0, slots)],
            dst_ref=level.at[pl.ds(tiles, slots)],
            send_sem=halo_send.at[index, 0],
            recv_sem=halo_recv.at[index, 0],
            device_id=(lax.rem(p + 1, parts), my),
            device_id_type=MESH,
        )
        down = pltpu.make_async_remote_copy(
            src_ref=sends.at[index, pl.ds(slots, slots)],
            dst_ref=level.at[pl.ds(tiles + slots, slots)],
            send_sem=halo_send.at[index, 1],
            recv_sem=halo_recv.at[index, 1],
            device_id=(lax.rem(p + parts - 1, parts), my),
            device_id_type=MESH,
        )
        return up, down

    def start_halo(index, level):
        up, down = halo(index, level)
        pl.when(has_up)(up.start)
        pl.when(has_low)(down.start)

    def wait_halo(index, level):
        up, down = halo(index, level)
        pl.when(has_low)(up.wait_recv)
        pl.when(has_up)(down.wait_recv)
        pl.when(has_up)(up.wait_send)
        pl.when(has_low)(down.wait_send)

    start_halo(0, level0)

    center = (high_ref[0] + low_ref[0]) * 0.5
    half_width = (high_ref[0] - low_ref[0]) * 0.5
    scale = jnp.ones((1, size), jnp.float32) / jnp.full((1, size), half_width, jnp.float32)

    def product(level, t):
        field = jnp.concatenate([level[cols[k, t]] for k in range(nnz)], axis=1)
        stored = jnp.concatenate([a_ref[t, k] for k in range(nnz)], axis=1)
        return lax.dot_general(field, stored, NT, preferred_element_type=jnp.float32)

    def first(t):
        own = level0[t].astype(jnp.float32)
        return ((product(level0, t) - center * own) * scale).astype(jnp.bfloat16)

    def second(t):
        own = level1[t].astype(jnp.float32)
        before = level0[t].astype(jnp.float32)
        return (2.0 * (product(level1, t) - center * own) * scale - before).astype(jnp.bfloat16)

    def send_tiles(index, make):
        @pl.loop(0, slots // 2)
        def _(i):
            made = []
            for u in range(2):
                s = i * 2 + u
                made.append((s, make(rows[1, s])))
                made.append((slots + s, make(rows[0, s])))
            for s, value in made:
                sends[index, s] = value

    def all_tiles(make, target, begin, count, group=4):
        @pl.loop(0, count // group)
        def _(i):
            made = [make(begin + i * group + u) for u in range(group)]
            for u in range(group):
                target[begin + i * group + u] = made[u]

    for load in loads:
        load.wait()
    wait_halo(0, level0)
    send_tiles(1, first)
    start_halo(1, level1)
    all_tiles(first, level1, 0, tiles)
    wait_halo(1, level1)
    send_tiles(2, second)
    start_halo(2, level2)

    def exchange(c):
        span = pl.ds(c * part_rows, part_rows)
        return pltpu.make_async_remote_copy(
            src_ref=level2.at[span],
            dst_ref=other.at[span],
            send_sem=mode_send.at[c],
            recv_sem=mode_recv.at[c],
            device_id=(p, 1 - my),
            device_id_type=MESH,
        )

    for c in range(chunks):
        all_tiles(second, level2, c * part_rows, part_rows)
        exchange(c).start()
    wait_halo(2, level2)
    all_tiles(lambda t: product(level2, t).astype(jnp.bfloat16), image, 0, tiles)

    total = jnp.zeros((width, width), jnp.float32)
    for c in range(chunks):
        exchange(c).wait_recv()

        def accumulate(i, acc):
            left, right = [], []
            for u in range(4):
                t = c * part_rows + i * 4 + u
                left.append(jnp.concatenate([level2[t], image[t]], axis=0))
                right.append(jnp.concatenate([level2[t], other[t]], axis=0))
            return acc + lax.dot_general(
                jnp.concatenate(left, axis=1), jnp.concatenate(right, axis=1), NT,
                preferred_element_type=jnp.float32,
            )

        total = lax.fori_loop(0, part_rows // 4, accumulate, total)
    total = jnp.where(my == 1, pltpu.roll(total, modes, 1), total)

    for s in range(stages + 1):
        partner = (flipped(1 << s), my) if s < stages else (p, 1 - my)
        ar_send[s] = total
        copy = pltpu.make_async_remote_copy(
            src_ref=ar_send.at[s],
            dst_ref=ar_recv.at[s],
            send_sem=ar_ssem.at[s],
            recv_sem=ar_rsem.at[s],
            device_id=partner,
            device_id_type=MESH,
        )
        copy.start()
        copy.wait()
        if s < stages:
            total = total + ar_recv[s]
    theirs = ar_recv[stages]
    count = parts * tiles * size
    lower = jnp.where(my == 0, total, theirs) / count
    upper = jnp.where(my == 0, theirs, total) / count
    gram = jnp.concatenate([lower[:modes], upper[:modes]], axis=0)
    projected_t = jnp.concatenate([lower[modes:], upper[modes:]], axis=0)

    step = 16
    row_id = lax.broadcasted_iota(jnp.int32, (width, width), 0)
    col_id = lax.broadcasted_iota(jnp.int32, (width, width), 1)
    work[:, :width] = gram
    work[:, width:] = (row_id == col_id).astype(jnp.float32)
    small = lax.broadcasted_iota(jnp.int32, (step, 1), 0)
    lanes = lax.broadcasted_iota(jnp.int32, (step, width), 1)

    @pl.loop(0, width // step)
    def _(b):
        begin = pl.multiple_of(b * step, step)
        panel = work[pl.ds(begin, step), :]
        near = panel[:, :width]
        columns = [
            jnp.sum(jnp.where(lanes == begin + s, near, 0.0), axis=1, keepdims=True)
            for s in range(step)
        ]
        pivots = jnp.zeros((step, 1), jnp.float32)
        for q in range(step):
            pivot = columns[q][q : q + 1, :]
            pivots = jnp.where(small == q, pivot, pivots)
            if q == step - 1:
                break
            factor = jnp.where(small > q, columns[q] / pivot, 0.0)
            panel = panel - factor * panel[q : q + 1, :]
            for s in range(q + 1, step):
                columns[s] = columns[s] - factor * columns[s][q : q + 1, :]
        inv_ref[pl.ds(begin, step), :] = panel[:, width:] / jnp.sqrt(pivots)
        below = jnp.where(lanes >= begin + step, panel[:, :width] / pivots, 0.0)
        work[...] = work[...] - lax.dot_general(
            below, panel, TN, precision=EXACT, preferred_element_type=jnp.float32
        )

    inverse = inv_ref[...]
    half = lax.dot_general(
        inverse, projected_t, NT, precision=EXACT, preferred_element_type=jnp.float32
    )
    ritz_ref[...] = lax.dot_general(
        half, inverse, NT, precision=EXACT, preferred_element_type=jnp.float32
    )
    own = jnp.where(my == 0, inverse[:modes], pltpu.roll(inverse[modes:], modes, 1))
    inv_t[...] = own.astype(jnp.bfloat16)
    for t in range(0, tiles, 2):
        pair = jnp.concatenate(
            [jnp.concatenate([level2[u], other[u]], axis=0) for u in (t, t + 1)], axis=1
        )
        basis_ref[:, t * size : (t + 2) * size] = lax.dot_general(
            inv_t[...], pair, NN, preferred_element_type=jnp.float32
        ).astype(jnp.bfloat16)
    for c in range(chunks):
        exchange(c).wait_send()


def shards(parts, stiffness_tiles, tile_cols, send_rows, block, lower_bound, upper_bound):
    row_count, modes = block.shape
    tiles, nnz, size = stiffness_tiles.shape[:3]
    slots = send_rows.shape[1]
    width = 2 * modes
    stages = parts.bit_length() - 1
    assert 1 << stages == parts
    chunks = 4
    smem = pl.BlockSpec(memory_space=pltpu.SMEM)
    vmem = pl.BlockSpec(memory_space=pltpu.VMEM)
    dma = pltpu.SemaphoreType.DMA
    level = pltpu.VMEM((tiles + 2 * slots, modes, size), jnp.bfloat16)
    field = pltpu.VMEM((tiles, modes, size), jnp.bfloat16)
    basis, ritz = pl.pallas_call(
        functools.partial(kernel, parts),
        out_shape=(
            jax.ShapeDtypeStruct((modes, row_count), jnp.bfloat16),
            jax.ShapeDtypeStruct((width, width), jnp.float32),
        ),
        in_specs=[smem, smem, smem, smem, vmem, pl.BlockSpec(memory_space=pl.ANY)],
        out_specs=(vmem, vmem),
        scratch_shapes=[
            pltpu.VMEM(stiffness_tiles.shape, jnp.bfloat16),
            level, level, level, field, field, field,
            pltpu.VMEM((3, 2 * slots, modes, size), jnp.bfloat16),
            pltpu.VMEM((stages + 1, width, width), jnp.float32),
            pltpu.VMEM((stages + 1, width, width), jnp.float32),
            pltpu.VMEM((width, 2 * width), jnp.float32),
            pltpu.VMEM((width, width), jnp.float32),
            pltpu.VMEM((modes, width), jnp.bfloat16),
            dma((4,)), dma((3, 2)), dma((3, 2)), dma((chunks,)), dma((chunks,)),
            dma((stages + 1,)), dma((stages + 1,)),
        ],
        compiler_params=pltpu.CompilerParams(
            collective_id=0, has_side_effects=True, vmem_limit_bytes=60 * 1024 * 1024
        ),
    )(tile_cols.T, send_rows, lower_bound, upper_bound, block.T, stiffness_tiles)
    return basis.T, ritz


def solution(mesh):
    placed = (
        P("dof", None, None, None),
        P("dof", None),
        P("dof", None),
        P("dof", "mode"),
        P(),
        P(),
    )
    return jax.shard_map(
        functools.partial(shards, mesh.shape["dof"]),
        mesh=mesh, in_specs=placed, out_specs=(P("dof", "mode"), P()), check_vma=False,
    )
```

```python
import functools

import jax
import jax.numpy as jnp
from jax import lax
from jax.experimental import pallas as pl
from jax.experimental.pallas import tpu as pltpu
from jax.sharding import PartitionSpec as P

MESH = pl.DeviceIdType.MESH
NT = (((1,), (1,)), ((), ()))
NN = (((1,), (0,)), ((), ()))
TN = (((0,), (0,)), ((), ()))
EXACT = lax.Precision.HIGHEST


def kernel(
    parts, cols, rows, low_ref, high_ref, x_ref, a_hbm, basis_ref, ritz_ref,
    a_ref, level0, level1, level2, plain, image, other, sends, ar_send, ar_recv,
    whole, final_send, final_recv, work, inv_ref, inv_t,
    a_sem, halo_send, halo_recv, mode_send, mode_recv, ar_ssem, ar_rsem,
):
    tiles, nnz, size = a_ref.shape[0], a_ref.shape[1], a_ref.shape[2]
    modes = x_ref.shape[0]
    width = 2 * modes
    slots = rows.shape[1]
    stages = ar_send.shape[0] - 1
    chunks = mode_send.shape[0]
    part_rows = tiles // chunks
    p = lax.axis_index("dof")
    my = lax.axis_index("mode")
    has_low = p > 0
    has_up = p < parts - 1

    loads = []
    a_parts = a_sem.shape[0]
    for i in range(a_parts):
        span = pl.ds(i * (tiles // a_parts), tiles // a_parts)
        loads.append(pltpu.make_async_copy(a_hbm.at[span], a_ref.at[span], a_sem.at[i]))
        loads[-1].start()

    def flipped(bit):
        return p + bit * (1 - 2 * ((p // bit) % 2))

    barrier = pltpu.get_barrier_semaphore()
    for s in range(stages):
        pl.semaphore_signal(barrier, inc=1, device_id=(flipped(1 << s), my), device_id_type=MESH)
    pl.semaphore_signal(barrier, inc=1, device_id=(p, 1 - my), device_id_type=MESH)

    @pl.when(has_low)
    def _():
        pl.semaphore_signal(barrier, inc=1, device_id=(p - 1, my), device_id_type=MESH)

    @pl.when(has_up)
    def _():
        pl.semaphore_signal(barrier, inc=1, device_id=(p + 1, my), device_id_type=MESH)

    for t in range(tiles):
        tile = x_ref[:, t * size : (t + 1) * size]
        level0[t] = tile
        plain[t] = tile

    @pl.when(p == 0)
    def _():
        for level in (level0, level1, level2):
            level[tiles : tiles + slots] = jnp.zeros((slots, modes, size), jnp.bfloat16)

    @pl.when(p == parts - 1)
    def _():
        for level in (level0, level1, level2):
            level[tiles + slots :] = jnp.zeros((slots, modes, size), jnp.bfloat16)

    for s in range(slots):
        sends[0, s] = plain[rows[1, s]]
        sends[0, slots + s] = plain[rows[0, s]]

    pl.semaphore_wait(
        barrier, stages + 1 + has_low.astype(jnp.int32) + has_up.astype(jnp.int32)
    )

    def halo(index, level):
        up = pltpu.make_async_remote_copy(
            src_ref=sends.at[index, pl.ds(0, slots)],
            dst_ref=level.at[pl.ds(tiles, slots)],
            send_sem=halo_send.at[index, 0],
            recv_sem=halo_recv.at[index, 0],
            device_id=(lax.rem(p + 1, parts), my),
            device_id_type=MESH,
        )
        down = pltpu.make_async_remote_copy(
            src_ref=sends.at[index, pl.ds(slots, slots)],
            dst_ref=level.at[pl.ds(tiles + slots, slots)],
            send_sem=halo_send.at[index, 1],
            recv_sem=halo_recv.at[index, 1],
            device_id=(lax.rem(p + parts - 1, parts), my),
            device_id_type=MESH,
        )
        return up, down

    def start_halo(index, level):
        up, down = halo(index, level)
        pl.when(has_up)(up.start)
        pl.when(has_low)(down.start)

    def wait_halo(index, level):
        up, down = halo(index, level)
        pl.when(has_low)(up.wait_recv)
        pl.when(has_up)(down.wait_recv)
        pl.when(has_up)(up.wait_send)
        pl.when(has_low)(down.wait_send)

    start_halo(0, level0)

    center = (high_ref[0] + low_ref[0]) * 0.5
    half_width = (high_ref[0] - low_ref[0]) * 0.5
    scale = jnp.ones((1, size), jnp.float32) / jnp.full((1, size), half_width, jnp.float32)

    def product(level, t):
        field = jnp.concatenate([level[cols[k, t]] for k in range(nnz)], axis=1)
        stored = jnp.concatenate([a_ref[t, k] for k in range(nnz)], axis=1)
        return lax.dot_general(field, stored, NT, preferred_element_type=jnp.float32)

    def first(t):
        own = level0[t].astype(jnp.float32)
        return ((product(level0, t) - center * own) * scale).astype(jnp.bfloat16)

    def second(t):
        own = level1[t].astype(jnp.float32)
        before = level0[t].astype(jnp.float32)
        return (2.0 * (product(level1, t) - center * own) * scale - before).astype(jnp.bfloat16)

    def send_tiles(index, make):
        @pl.loop(0, slots // 2)
        def _(i):
            made = []
            for u in range(2):
                s = i * 2 + u
                made.append((s, make(rows[1, s])))
                made.append((slots + s, make(rows[0, s])))
            for s, value in made:
                sends[index, s] = value

    def all_tiles(make, target, begin, count, group=4):
        @pl.loop(0, count // group)
        def _(i):
            made = [make(begin + i * group + u) for u in range(group)]
            for u in range(group):
                target[begin + i * group + u] = made[u]

    for load in loads:
        load.wait()
    wait_halo(0, level0)
    send_tiles(1, first)
    start_halo(1, level1)
    all_tiles(first, level1, 0, tiles)
    wait_halo(1, level1)
    send_tiles(2, second)
    start_halo(2, level2)

    def exchange(c):
        span = pl.ds(c * part_rows, part_rows)
        return pltpu.make_async_remote_copy(
            src_ref=level2.at[span],
            dst_ref=other.at[span],
            send_sem=mode_send.at[c],
            recv_sem=mode_recv.at[c],
            device_id=(p, 1 - my),
            device_id_type=MESH,
        )

    for c in range(chunks):
        all_tiles(second, level2, c * part_rows, part_rows)
        exchange(c).start()
    wait_halo(2, level2)
    all_tiles(lambda t: product(level2, t).astype(jnp.bfloat16), image, 0, tiles)

    total = jnp.zeros((width, width), jnp.float32)
    for c in range(chunks):
        exchange(c).wait_recv()

        def accumulate(i, acc):
            left, right = [], []
            for u in range(4):
                t = c * part_rows + i * 4 + u
                left.append(jnp.concatenate([level2[t], image[t]], axis=0))
                right.append(jnp.concatenate([level2[t], other[t]], axis=0))
            return acc + lax.dot_general(
                jnp.concatenate(left, axis=1), jnp.concatenate(right, axis=1), NT,
                preferred_element_type=jnp.float32,
            )

        total = lax.fori_loop(0, part_rows // 4, accumulate, total)
    total = jnp.where(my == 1, pltpu.roll(total, modes, 1), total)

    core = lax.rem(p, 2)
    start_own = pl.multiple_of(core * modes, modes)
    start_out = pl.multiple_of((1 - core) * modes, modes)
    whole[...] = total

    def transfer(s, source, target, partner):
        copy = pltpu.make_async_remote_copy(
            src_ref=source,
            dst_ref=target,
            send_sem=ar_ssem.at[s],
            recv_sem=ar_rsem.at[s],
            device_id=partner,
            device_id_type=MESH,
        )
        copy.start()
        copy.wait()

    transfer(0, whole.at[pl.ds(start_out, modes)], ar_recv.at[0], (flipped(1), my))
    part = whole[pl.ds(start_own, modes), :] + ar_recv[0]
    for s in range(1, stages + 1):
        partner = (flipped(1 << s), my) if s < stages else (p, 1 - my)
        ar_send[s] = part
        transfer(s, ar_send.at[s], ar_recv.at[s], partner)
        if s < stages:
            part = part + ar_recv[s]
    theirs = ar_recv[stages]
    low_part = jnp.where(my == 0, part, theirs)
    high_part = jnp.where(my == 0, theirs, part)
    final_send[:modes] = low_part
    final_send[modes:] = high_part
    transfer(stages + 1, final_send, final_recv, (flipped(1), my))
    mine, received = final_send[...], final_recv[...]
    count = parts * tiles * size
    gram = jnp.where(core == 0, mine, received) / count
    projected_t = jnp.where(core == 0, received, mine) / count

    step = 16
    row_id = lax.broadcasted_iota(jnp.int32, (width, width), 0)
    col_id = lax.broadcasted_iota(jnp.int32, (width, width), 1)
    work[:, :width] = gram
    work[:, width:] = (row_id == col_id).astype(jnp.float32)
    small = lax.broadcasted_iota(jnp.int32, (step, 1), 0)
    lanes = lax.broadcasted_iota(jnp.int32, (step, width), 1)

    @pl.loop(0, width // step)
    def _(b):
        begin = pl.multiple_of(b * step, step)
        panel = work[pl.ds(begin, step), :]
        near = panel[:, :width]
        columns = [
            jnp.sum(jnp.where(lanes == begin + s, near, 0.0), axis=1, keepdims=True)
            for s in range(step)
        ]
        pivots = jnp.zeros((step, 1), jnp.float32)
        for q in range(step):
            pivot = columns[q][q : q + 1, :]
            pivots = jnp.where(small == q, pivot, pivots)
            if q == step - 1:
                break
            factor = jnp.where(small > q, columns[q] / pivot, 0.0)
            panel = panel - factor * panel[q : q + 1, :]
            for s in range(q + 1, step):
                columns[s] = columns[s] - factor * columns[s][q : q + 1, :]
        inv_ref[pl.ds(begin, step), :] = panel[:, width:] / jnp.sqrt(pivots)
        below = jnp.where(lanes >= begin + step, panel[:, :width] / pivots, 0.0)
        work[...] = work[...] - lax.dot_general(
            below, panel, TN, precision=EXACT, preferred_element_type=jnp.float32
        )

    inverse = inv_ref[...]
    half = lax.dot_general(
        inverse, projected_t, NT, precision=EXACT, preferred_element_type=jnp.float32
    )
    ritz_ref[...] = lax.dot_general(
        half, inverse, NT, precision=EXACT, preferred_element_type=jnp.float32
    )
    own = jnp.where(my == 0, inverse[:modes], pltpu.roll(inverse[modes:], modes, 1))
    inv_t[...] = own.astype(jnp.bfloat16)
    for t in range(0, tiles, 2):
        pair = jnp.concatenate(
            [jnp.concatenate([level2[u], other[u]], axis=0) for u in (t, t + 1)], axis=1
        )
        basis_ref[:, t * size : (t + 2) * size] = lax.dot_general(
            inv_t[...], pair, NN, preferred_element_type=jnp.float32
        ).astype(jnp.bfloat16)
    for c in range(chunks):
        exchange(c).wait_send()


def shards(parts, stiffness_tiles, tile_cols, send_rows, block, lower_bound, upper_bound):
    row_count, modes = block.shape
    tiles, nnz, size = stiffness_tiles.shape[:3]
    slots = send_rows.shape[1]
    width = 2 * modes
    stages = parts.bit_length() - 1
    assert 1 << stages == parts
    chunks = 4
    smem = pl.BlockSpec(memory_space=pltpu.SMEM)
    vmem = pl.BlockSpec(memory_space=pltpu.VMEM)
    dma = pltpu.SemaphoreType.DMA
    level = pltpu.VMEM((tiles + 2 * slots, modes, size), jnp.bfloat16)
    field = pltpu.VMEM((tiles, modes, size), jnp.bfloat16)
    basis, ritz = pl.pallas_call(
        functools.partial(kernel, parts),
        out_shape=(
            jax.ShapeDtypeStruct((modes, row_count), jnp.bfloat16),
            jax.ShapeDtypeStruct((width, width), jnp.float32),
        ),
        in_specs=[smem, smem, smem, smem, vmem, pl.BlockSpec(memory_space=pl.ANY)],
        out_specs=(vmem, vmem),
        scratch_shapes=[
            pltpu.VMEM(stiffness_tiles.shape, jnp.bfloat16),
            level, level, level, field, field, field,
            pltpu.VMEM((3, 2 * slots, modes, size), jnp.bfloat16),
            pltpu.VMEM((stages + 1, modes, width), jnp.float32),
            pltpu.VMEM((stages + 1, modes, width), jnp.float32),
            pltpu.VMEM((width, width), jnp.float32),
            pltpu.VMEM((width, width), jnp.float32),
            pltpu.VMEM((width, width), jnp.float32),
            pltpu.VMEM((width, 2 * width), jnp.float32),
            pltpu.VMEM((width, width), jnp.float32),
            pltpu.VMEM((modes, width), jnp.bfloat16),
            dma((4,)), dma((3, 2)), dma((3, 2)), dma((chunks,)), dma((chunks,)),
            dma((stages + 2,)), dma((stages + 2,)),
        ],
        compiler_params=pltpu.CompilerParams(
            collective_id=0, has_side_effects=True, vmem_limit_bytes=60 * 1024 * 1024
        ),
    )(tile_cols.T, send_rows, lower_bound, upper_bound, block.T, stiffness_tiles)
    return basis.T, ritz


def solution(mesh):
    placed = (
        P("dof", None, None, None),
        P("dof", None),
        P("dof", None),
        P("dof", "mode"),
        P(),
        P(),
    )
    return jax.shard_map(
        functools.partial(shards, mesh.shape["dof"]),
        mesh=mesh, in_specs=placed, out_specs=(P("dof", "mode"), P()), check_vma=False,
    )
```
